128 devices in a mesh: lat: 16 (over x, z_lo, core), lon: 8 (over z_hi, y).
Axes of the slice: x: 4, y: 4, z: 4 (z_hi: 2, z_lo: 2; z = z_hi * 2 + z_lo), core: 2. Of those that a mesh axis runs over, the one named last changes fastest.
Arguments:
- current: bfloat16 [69, 512, 1024], P(None, 'lat', 'lon')
- next_fields: bfloat16 [128, 512, 1024], P(('lat', 'lon')), may hold values from -6 to 6
- reader_slot: int32 [69], replicated, may hold values from 0 to 127, as said below
- first_weight: bfloat16 [9, 256, 69], replicated, may hold values from -0.25 to 0.25
- first_bias: float32 [256], replicated, may hold values from -3 to 3
- second_weight: bfloat16 [9, 256, 256], replicated, may hold values from -0.125 to 0.125
- second_bias: float32 [256], replicated, may hold values from -3 to 3
Outputs:
- features: bfloat16 [256, 512, 1024], P(None, 'lat', 'lon')
- next_tile: bfloat16 [69, 512, 1024], P(None, 'lat', 'lon')
The draws below stay inside these ranges and needn't reach their ends.
Inputs may be any that keep to these rules, and one draw needn't show every extreme that they name: `reader_slot`: the 69 entries are different slots.
All inputs are finite; a program needn't handle non-finite values.
Results may differ from the reference program's by a relative error of at most 0.0053.
Values may be sent and summed in bfloat16 or wider, within the bound.
A program may use at most 128 MiB of HBM per device.

```python
import jax
import jax.numpy as jnp
from jax import lax

C = 69
HID = 256
LAT_DEV = 32
LON_DEV = 128
H = 512
W = 1024
SLOTS = 128


def draw_current(key, part):
    keys = jax.random.split(jax.random.fold_in(key, 11), 7)
    profile = (jnp.arange(H, dtype=jnp.float32) / (H - 1))[None, :, None]
    rough = jax.random.uniform(keys[4], (C, 1, W), jnp.float32, 0.5, 1.5)
    slope = jax.random.uniform(keys[2], (C, 1, 1), jnp.float32, -2.0, 2.0)
    lat_tiles = H // LAT_DEV
    lon_tiles = W // LON_DEV
    tile_level = jax.random.normal(keys[5], (C, lat_tiles, 1, lon_tiles, 1), jnp.float32)
    tile_field = jnp.broadcast_to(tile_level, (C, lat_tiles, LAT_DEV, lon_tiles, LON_DEV)).reshape(C, H, W)
    half_level = jax.random.normal(keys[6], (C, 1, 2), jnp.float32)
    half_field = jnp.repeat(half_level, W // 2, axis=2)
    noise = jax.random.normal(keys[0], (C, H, W), jnp.float32)
    offset = jax.random.normal(keys[1], (C, 1, 1), jnp.float32)
    spread = 1.0 + 2.0 * profile
    tile_scale = 0.8
    values = offset + 3.0 * slope * profile + tile_scale * tile_field + half_field + spread * rough * noise
    return values.astype(jnp.bfloat16)


def draw_reader_slot(key, part):
    order = jax.random.permutation(jax.random.fold_in(key, 23), SLOTS)
    return order[:C].astype(jnp.int32)


def steps_of(rng, shape, shards, smallest, top_value):
    loudness = 1.0
    for dim, shards_of in shards:
        heights = jax.random.uniform(jax.random.fold_in(jax.random.fold_in(rng, 6), dim), (shards_of,), jnp.float32, smallest / len(shards), top_value / len(shards))
        loudness = loudness * jnp.repeat(jnp.exp(heights), shape[dim] // shards_of).reshape((-1,) + (1,) * (len(shape) - 1 - dim))
    return loudness


def scatter_about(own_key, dims, scale, most, cuts=(), held_as=jnp.bfloat16):
    level = steps_of(own_key, dims, cuts, -0.22, 0.18) if cuts else 1.0
    drawn = jax.random.normal(own_key, dims, jnp.float32) * scale * level
    return jnp.minimum(jnp.maximum(drawn, -most), most).astype(held_as)


def setup_inputs(seed: int = 0) -> dict:
    key_of = jax.random.split(jax.random.key(seed), 8)
    current = draw_current(jax.random.fold_in(key_of[7], 71), 0)
    next_fields = scatter_about(key_of[1], (SLOTS, H, W), 1.0, 6.0, ((0, 128),))
    reader_slot = draw_reader_slot(jax.random.fold_in(key_of[7], 71), 0)
    first_weight = scatter_about(key_of[3], (9, HID, C), (9 * C) ** -0.5, 0.25)
    first_bias = scatter_about(key_of[4], (HID,), 0.5, 3.0, (), jnp.float32)
    second_weight = scatter_about(key_of[5], (9, HID, HID), (9 * HID) ** -0.5, 0.125)
    second_bias = scatter_about(key_of[6], (HID,), 0.5, 3.0, (), jnp.float32)
    return {"current": current, "next_fields": next_fields, "reader_slot": reader_slot, "first_weight": first_weight, "first_bias": first_bias, "second_weight": second_weight, "second_bias": second_bias}


def conv_grid(field, weight):
    padded = jnp.pad(field.astype(jnp.float32), ((0, 0), (1, 1), (0, 0)))
    padded = jnp.concatenate([padded[:, :, -1:], padded, padded[:, :, :1]], axis=2)
    rows = field.shape[1]
    cols = field.shape[2]
    total = jnp.zeros((weight.shape[1], rows, cols), jnp.float32)
    for tap in range(9):
        shifted = padded[:, tap // 3:tap // 3 + rows, tap % 3:tap % 3 + cols]
        total = total + jnp.einsum('ok,khw->ohw', weight[tap].astype(jnp.float32), shifted)
    return total

def reference(current, next_fields, reader_slot, first_weight, first_bias, second_weight, second_bias):
    values = current.astype(jnp.float32)
    cells = values.shape[1] * values.shape[2]
    mean = lax.optimization_barrier(jnp.sum(values, axis=(1, 2))) / cells
    square = lax.optimization_barrier(jnp.sum(values * values, axis=(1, 2))) / cells
    scale = 1.0 / jnp.sqrt(square - mean * mean + 1e-05)
    normed = ((values - mean[:, None, None]) * scale[:, None, None]).astype(jnp.bfloat16)
    hidden = jax.nn.gelu(conv_grid(normed, first_weight) + first_bias[:, None, None], approximate=True).astype(jnp.bfloat16)
    features = (conv_grid(hidden, second_weight) + second_bias[:, None, None]).astype(jnp.bfloat16)
    next_tile = jnp.take(next_fields, reader_slot, axis=0)
    return (features, next_tile)
```

```python
import functools
import random

import jax
import jax.numpy as jnp
from jax import lax
from jax.experimental import pallas as pl
from jax.experimental.pallas import tpu as pltpu
from jax.sharding import PartitionSpec as P

MESH = pl.DeviceIdType.MESH
KB = 80
KP = 256


def gelu(v):
    u = v * (0.7978845608028654 + 0.035677408136300125 * (v * v))
    half = 0.5 * v
    return half + half * jnp.tanh(u)


def kernel(n_lat, n_lon, channels, rows, cols, hid_ch,
           cur_hbm, nf_hbm, slot_hbm, w1_hbm, b1_hbm, w2_hbm, b2_hbm,
           feat_ref, next_ref,
           cur, w1, w2, bv, slot, tt, aa, sa, xx, xe, w1c, w1s, bias, hid, edge,
           stat, srecv, recv, in_sem, h_send, h_recv, s_send, s_recv, a_send, a_recv):
    f32, bf16 = jnp.float32, jnp.bfloat16
    n_dev = n_lat * n_lon
    lat = lax.axis_index("lat")
    lon = lax.axis_index("lon")
    me = lat * n_lon + lon
    la = [lax.rem(lat + d, n_lat) for d in range(n_lat)]
    lo = [lax.rem(lon + d, n_lon) for d in range(n_lon)]
    order = [(a, b) for a in range(n_lat) for b in range(n_lon) if (a, b) != (0, 0)]
    random.Random(0).shuffle(order)

    def load(i, src, dst):
        return pltpu.make_async_copy(src, dst, in_sem.at[i])

    loads = [load(0, cur_hbm, cur), load(1, w1_hbm, w1), load(2, b1_hbm, bv.at[0]),
             load(3, b2_hbm, bv.at[1]), load(4, w2_hbm, w2), load(5, slot_hbm, slot)]
    for c in loads:
        c.start()
    own = pltpu.make_async_copy(
        nf_hbm.at[0, pl.ds(pl.multiple_of(lat * rows, rows), rows), pl.ds(pl.multiple_of(lon * cols, cols), cols)],
        recv.at[me], in_sem.at[6])
    own.start()
    barrier = pltpu.get_barrier_semaphore()
    for a, b in order:
        pl.semaphore_signal(barrier, inc=1, device_id=(la[a], lo[b]), device_id_type=MESH)

    tt[2:rows + 2, 64:KB, :] = jnp.zeros((rows, KB - 64, cols), bf16)
    loads[0].wait()
    sum1 = jnp.zeros((channels, cols), f32)
    sum2 = jnp.zeros((channels, cols), f32)
    for h in range(0, rows, 8):
        t = jnp.swapaxes(cur[:, h:h + 8, :].astype(f32), 0, 1)
        sum1 = sum1 + jnp.sum(t, axis=0)
        sum2 = sum2 + jnp.sum(t * t, axis=0)
        tt[2 + h:10 + h, 0:channels, :] = t.astype(bf16)
    diag = lax.broadcasted_iota(jnp.int32, (channels, cols), 0) == lax.broadcasted_iota(jnp.int32, (channels, cols), 1)
    for i, s in enumerate((sum1, sum2)):
        col = jnp.sum(s, axis=1, keepdims=True)
        stat[i:i + 1, :] = jnp.sum(jnp.where(diag, col, 0.0), axis=0, keepdims=True)
    lane = lax.broadcasted_iota(jnp.int32, (KB, cols), 1)
    lane_row = lax.shift_right_logical(lane * 171, 9)
    lane_col = lane - 3 * lane_row

    def strips(first, last, base):
        out = list(base)
        for r in range(first, last):
            v = tt[r]
            for s in range(2):
                out[s] = jnp.where(lane_row == r, pltpu.roll(v, (3 * r + 2 - s) % cols, axis=1), out[s])
        return out

    zero = jnp.zeros((KB, cols), bf16)
    strip = strips(2, rows + 2, (zero, zero))
    aa[0] = strip[0]
    aa[1] = strip[1]
    loads[1].wait()
    w1c[...] = jnp.zeros_like(w1c)
    for tap in range(9):
        w1c[tap // 3, :, KB * (tap % 3):KB * (tap % 3) + channels] = w1[tap]
    xx[:, 3 * KB:KP, :] = jnp.zeros((rows + 4, KP - 3 * KB, cols), bf16)
    xe[:, :, 3 * KB:KP, :] = jnp.zeros((3, 2, KP - 3 * KB, cols), bf16)
    loads[2].wait()
    loads[3].wait()
    eye = lax.broadcasted_iota(jnp.int32, (hid_ch, hid_ch), 0) == lax.broadcasted_iota(jnp.int32, (hid_ch, hid_ch), 1)
    for i in range(2):
        col = jnp.sum(jnp.where(eye, bv[i], 0.0), axis=1, keepdims=True)
        bias[i] = jnp.broadcast_to(col, (hid_ch, cols))
    srecv[me] = stat[...]
    pl.semaphore_wait(barrier, n_dev - 1)

    up, down, east, west = la[n_lat - 1], la[1], lo[1], lo[n_lon - 1]
    halo = [
        (aa.at[0], sa.at[0], lat, east), (aa.at[0], sa.at[1], up, east), (aa.at[0], sa.at[2], down, east),
        (aa.at[1], sa.at[3], lat, west), (aa.at[1], sa.at[4], up, west), (aa.at[1], sa.at[5], down, west),
        (tt.at[pl.ds(2, 2)], tt.at[pl.ds(rows + 2, 2)], up, lon), (tt.at[pl.ds(rows, 2)], tt.at[pl.ds(0, 2)], down, lon),
    ]
    sent = []
    for i, (src, dst, p, q) in enumerate(halo):
        c = pltpu.make_async_remote_copy(src, dst, h_send.at[i], h_recv.at[i], device_id=(p, q), device_id_type=MESH)
        c.start()
        sent.append(c)
    for a, b in order:
        pltpu.make_async_remote_copy(stat, srecv.at[me], s_send, s_recv,
                                     device_id=(la[a], lo[b]), device_id_type=MESH).start()
    for a, b in order:
        pltpu.make_async_remote_copy(
            nf_hbm.at[0, pl.ds(pl.multiple_of(la[a] * rows, rows), rows), pl.ds(pl.multiple_of(lo[b] * cols, cols), cols)],
            recv.at[me], a_send, a_recv, device_id=(la[a], lo[b]), device_id_type=MESH).start()

    for c in sent:
        c.wait_recv()
    first = lat == 0
    last = lat == n_lat - 1
    for r in (0, 1):
        tt[r] = jnp.where(first, zero, tt[r])
        tt[rows + 2 + r] = jnp.where(last, zero, tt[rows + 2 + r])
    strip = strips(0, 2, strips(rows + 2, rows + 4, (aa[0], aa[1])))
    valid = (lane < 3 * (rows + 4)) & ((lane >= 6) | (lat > 0)) & ((lane < 3 * (rows + 2)) | (lat < n_lat - 1))
    shift = 3 * rows
    west_in = jnp.where(lane < 6, pltpu.roll(sa[2], cols - shift, axis=1),
                        jnp.where(lane < 3 * (rows + 2), sa[0], pltpu.roll(sa[1], shift, axis=1)))
    east_in = jnp.where(lane < 6, pltpu.roll(sa[5], cols - shift, axis=1),
                        jnp.where(lane < 3 * (rows + 2), sa[3], pltpu.roll(sa[4], shift, axis=1)))
    g_west = jnp.where(valid, jnp.where(lane_col == 2, strip[0], west_in), zero)
    g_east = jnp.where(valid, jnp.where(lane_col == 0, strip[1], east_in), zero)
    for a in range(3):
        for b in range(3):
            amount = (-(3 * (a - 1) + b - 1)) % cols
            for s, g in enumerate((g_west, g_east)):
                xe[a, s, KB * b:KB * (b + 1), :] = pltpu.roll(g, amount, axis=1) if amount else g
    for r in range(rows + 4):
        v = tt[r]
        center = 3 * r + 1
        xx[r, 0:KB, :] = jnp.where(lane == 0, pltpu.roll(g_west, (-center) % cols, axis=1), pltpu.roll(v, 1, axis=1))
        xx[r, KB:2 * KB, :] = v
        xx[r, 2 * KB:3 * KB, :] = jnp.where(
            lane == cols - 1, pltpu.roll(g_east, (cols - 1 - center) % cols, axis=1), pltpu.roll(v, cols - 1, axis=1))

    def drain(buf, sem):
        w = buf.at[pl.ds(0, n_dev - 1)]
        pltpu.make_async_copy(w, w, sem).wait()

    drain(srecv, s_recv)
    total = jnp.sum(srecv[...], axis=0) / (n_dev * rows * cols)
    mean = total[0:1, :]
    scale = 1.0 / jnp.sqrt(total[1:2, :] - mean * mean + 1e-05)
    in_use = lax.broadcasted_iota(jnp.int32, (1, cols), 1) < channels

    def beside(v):
        wide = jnp.concatenate([jnp.where(in_use, v, 0.0), jnp.zeros((1, KP - cols), f32)], axis=1)
        return wide + pltpu.roll(wide, KB, axis=1) + pltpu.roll(wide, 2 * KB, axis=1)

    mean_k, scale_k = beside(mean), beside(scale)
    full = bias[0]
    for a in range(3):
        ws = (w1c[a].astype(f32) * scale_k).astype(bf16)
        w1s[a] = ws
        part = jnp.broadcast_to(jnp.sum(ws.astype(f32) * mean_k, axis=1, keepdims=True), (hid_ch, cols))
        full = full - part
        if a != 1:
            bias[2 + a // 2] = part
    bias[0] = full

    top = jnp.where(first, 1.0, 0.0).astype(f32)
    bottom = jnp.where(last, 1.0, 0.0).astype(f32)
    hlane = lax.broadcasted_iota(jnp.int32, (hid_ch, cols), 1)

    def conv1(parts):
        acc = jnp.zeros((hid_ch, cols * len(parts(0))), f32)
        for a in range(3):
            acc = acc + jnp.dot(w1s[a], jnp.concatenate(parts(a), axis=1), preferred_element_type=f32)
        return acc

    def put(r, h):
        hid[1, r] = h
        center = 3 * (r + 1) + 1
        hid[0, r] = jnp.where(hlane == 0, pltpu.roll(edge[0], lax.rem(2 * cols - center, cols), axis=1), pltpu.roll(h, 1, axis=1))
        hid[2, r] = jnp.where(hlane == cols - 1, pltpu.roll(edge[1], lax.rem(2 * cols - 1 - center, cols), axis=1),
                              pltpu.roll(h, cols - 1, axis=1))

    acc = conv1(lambda a: [xe[a, 0], xe[a, 1], xx[rows + a], xx[rows + 1 + a]])
    ebias = (bias[0] + jnp.where((hlane >= 6) & (hlane < 9), top, 0.0) * bias[2]
             + jnp.where((hlane >= 3 * rows + 3) & (hlane < 3 * rows + 6), bottom, 0.0) * bias[3])
    keep = (((hlane >= 6) | (lat > 0)) & ((hlane < 3 * rows + 6) | (lat < n_lat - 1)))
    for s in range(2):
        edge[s] = jnp.where(keep, gelu(acc[:, s * cols:(s + 1) * cols] + ebias), 0.0).astype(bf16)
    put(rows, gelu(acc[:, 2 * cols:3 * cols] + (bias[0] + bottom * bias[3])).astype(bf16))
    put(rows + 1, jnp.where(last, 0.0, gelu(acc[:, 3 * cols:] + bias[0])).astype(bf16))

    def tile1(r0):
        acc = conv1(lambda a: [xx[r0 + a + q] for q in range(4)])
        for q in range(4):
            v = acc[:, q * cols:(q + 1) * cols] + bias[0]
            if r0 == 0 and q == 1:
                v = v + top * bias[2]
            h = gelu(v)
            if r0 == 0 and q == 0:
                h = jnp.where(first, 0.0, h)
            put(r0 + q, h.astype(bf16))

    def tile2(r0):
        acc = jnp.zeros((hid_ch, 4 * cols), f32)
        for a in range(3):
            for b in range(3):
                x = jnp.concatenate([hid[b, r0 + a + q] for q in range(4)], axis=1)
                acc = acc + jnp.dot(w2[3 * a + b], x, preferred_element_type=f32)
        return [acc[:, q * cols:(q + 1) * cols] + bias[1] for q in range(4)]

    loads[4].wait()
    for r0 in (0, 4, 8):
        tile1(r0)
    for g in range(rows // 8):
        for r0 in (8 * g + 12, 8 * g + 16):
            if r0 < rows:
                tile1(r0)
        outs = tile2(8 * g) + tile2(8 * g + 4)
        feat_ref[:, 8 * g:8 * g + 8, :] = jnp.swapaxes(jnp.stack(outs, axis=0), 0, 1).astype(bf16)

    own.wait()
    loads[5].wait()
    drain(recv, a_recv)
    for c in range(channels):
        next_ref[c] = recv[slot[c]]
    for c in sent:
        c.wait_send()
    drain(srecv, s_send)
    drain(recv, a_send)


def solution(mesh):
    n_lat, n_lon = mesh.shape["lat"], mesh.shape["lon"]
    n_dev = n_lat * n_lon

    def body(current, next_fields, reader_slot, first_weight, first_bias, second_weight, second_bias):
        channels, rows, cols = current.shape
        hid_ch = first_weight.shape[1]
        bf16, f32 = jnp.bfloat16, jnp.float32
        dma = pltpu.SemaphoreType.DMA
        return pl.pallas_call(
            functools.partial(kernel, n_lat, n_lon, channels, rows, cols, hid_ch),
            out_shape=(jax.ShapeDtypeStruct((hid_ch, rows, cols), bf16), jax.ShapeDtypeStruct((channels, rows, cols), bf16)),
            in_specs=[pl.BlockSpec(memory_space=pl.ANY)] * 7,
            out_specs=(pl.BlockSpec(memory_space=pltpu.VMEM),) * 2,
            scratch_shapes=[
                pltpu.VMEM((channels, rows, cols), bf16),
                pltpu.VMEM(first_weight.shape, bf16),
                pltpu.VMEM(second_weight.shape, bf16),
                pltpu.VMEM((2, 1, hid_ch), f32),
                pltpu.SMEM(reader_slot.shape, jnp.int32),
                pltpu.VMEM((rows + 4, KB, cols), bf16),
                pltpu.VMEM((2, KB, cols), bf16),
                pltpu.VMEM((6, KB, cols), bf16),
                pltpu.VMEM((rows + 4, KP, cols), bf16),
                pltpu.VMEM((3, 2, KP, cols), bf16),
                pltpu.VMEM((3, hid_ch, KP), bf16),
                pltpu.VMEM((3, hid_ch, KP), bf16),
                pltpu.VMEM((4, hid_ch, cols), f32),
                pltpu.VMEM((3, rows + 2, hid_ch, cols), bf16),
                pltpu.VMEM((2, hid_ch, cols), bf16),
                pltpu.VMEM((2, cols), f32),
                pltpu.VMEM((n_dev, 2, cols), f32),
                pltpu.VMEM((n_dev, rows, cols), bf16),
                dma((7,)), dma((8,)), dma((8,)), dma, dma, dma, dma,
            ],
            compiler_params=pltpu.CompilerParams(collective_id=0, has_side_effects=True, vmem_limit_bytes=40 * 1024 * 1024),
        )(current, next_fields, reader_slot, first_weight, first_bias.reshape(1, -1), second_weight, second_bias.reshape(1, -1))

    split = P(None, "lat", "lon")
    return jax.shard_map(
        body,
        mesh=mesh,
        in_specs=(split, P(("lat", "lon"), None, None), P(), P(), P(), P(), P()),
        out_specs=(split, split),
        check_vma=False,
    )
```

```python
import functools
import random

import jax
import jax.numpy as jnp
from jax import lax
from jax.experimental import pallas as pl
from jax.experimental.pallas import tpu as pltpu
from jax.sharding import PartitionSpec as P

MESH = pl.DeviceIdType.MESH
KB = 80
KP = 256


def gelu(v):
    u = v * (0.7978845608028654 + 0.035677408136300125 * (v * v))
    half = 0.5 * v
    return half + half * jnp.tanh(u)


def kernel(n_lat, n_lon, channels, rows, cols, hid_ch,
           cur_hbm, nf_hbm, slot_hbm, w1_hbm, b1_hbm, w2_hbm, b2_hbm,
           feat_ref, next_ref,
           cur, w1, w2, bv, slot, tt, aa, sa, xx, xe, w1c, w1s, bias, hid, edge,
           stat, srecv, recv, in_sem, h_send, h_recv, s_send, s_recv, a_send, a_recv):
    f32, bf16 = jnp.float32, jnp.bfloat16
    n_dev = n_lat * n_lon
    lat = lax.axis_index("lat")
    lon = lax.axis_index("lon")
    me = lat * n_lon + lon
    la = [lax.rem(lat + d, n_lat) for d in range(n_lat)]
    lo = [lax.rem(lon + d, n_lon) for d in range(n_lon)]
    order = [(a, b) for a in range(n_lat) for b in range(n_lon) if (a, b) != (0, 0)]
    random.Random(0).shuffle(order)

    def load(i, src, dst):
        return pltpu.make_async_copy(src, dst, in_sem.at[i])

    loads = [load(0, cur_hbm, cur), load(1, w1_hbm, w1), load(2, b1_hbm, bv.at[0]),
             load(3, b2_hbm, bv.at[1]), load(4, w2_hbm, w2), load(5, slot_hbm, slot)]
    for c in loads:
        c.start()
    own = pltpu.make_async_copy(
        nf_hbm.at[0, pl.ds(pl.multiple_of(lat * rows, rows), rows), pl.ds(pl.multiple_of(lon * cols, cols), cols)],
        recv.at[me], in_sem.at[6])
    own.start()
    barrier = pltpu.get_barrier_semaphore()
    for a, b in order:
        pl.semaphore_signal(barrier, inc=1, device_id=(la[a], lo[b]), device_id_type=MESH)

    tt[2:rows + 2, 64:KB, :] = jnp.zeros((rows, KB - 64, cols), bf16)
    loads[0].wait()
    sum1 = jnp.zeros((channels, cols), f32)
    sum2 = jnp.zeros((channels, cols), f32)
    for h in range(0, rows, 8):
        t = jnp.swapaxes(cur[:, h:h + 8, :].astype(f32), 0, 1)
        sum1 = sum1 + jnp.sum(t, axis=0)
        sum2 = sum2 + jnp.sum(t * t, axis=0)
        tt[2 + h:10 + h, 0:channels, :] = t.astype(bf16)
    diag = lax.broadcasted_iota(jnp.int32, (channels, cols), 0) == lax.broadcasted_iota(jnp.int32, (channels, cols), 1)
    for i, s in enumerate((sum1, sum2)):
        col = jnp.sum(s, axis=1, keepdims=True)
        stat[i:i + 1, :] = jnp.sum(jnp.where(diag, col, 0.0), axis=0, keepdims=True)
    lane = lax.broadcasted_iota(jnp.int32, (KB, cols), 1)
    lane_row = lax.shift_right_logical(lane * 171, 9)
    lane_col = lane - 3 * lane_row

    def strips(first, last, base):
        out = list(base)
        for r in range(first, last):
            v = tt[r]
            for s in range(2):
                out[s] = jnp.where(lane_row == r, pltpu.roll(v, (3 * r + 2 - s) % cols, axis=1), out[s])
        return out

    zero = jnp.zeros((KB, cols), bf16)
    strip = strips(2, rows + 2, (zero, zero))
    aa[0] = strip[0]
    aa[1] = strip[1]
    loads[1].wait()
    w1c[...] = jnp.zeros_like(w1c)
    for tap in range(9):
        w1c[tap // 3, KB * (tap % 3):KB * (tap % 3) + channels, :] = w1[tap]
    for a in range(3):
        w1c[a] = jnp.transpose(w1c[a])
    xx[:, 3 * KB:KP, :] = jnp.zeros((rows + 4, KP - 3 * KB, cols), bf16)
    xe[:, :, 3 * KB:KP, :] = jnp.zeros((3, 2, KP - 3 * KB, cols), bf16)
    loads[2].wait()
    loads[3].wait()
    eye = lax.broadcasted_iota(jnp.int32, (hid_ch, hid_ch), 0) == lax.broadcasted_iota(jnp.int32, (hid_ch, hid_ch), 1)
    for i in range(2):
        col = jnp.sum(jnp.where(eye, bv[i], 0.0), axis=1, keepdims=True)
        bias[i] = jnp.broadcast_to(col, (hid_ch, cols))
    srecv[me] = stat[...]
    pl.semaphore_wait(barrier, n_dev - 1)

    up, down, east, west = la[n_lat - 1], la[1], lo[1], lo[n_lon - 1]
    halo = [
        (aa.at[0], sa.at[0], lat, east), (aa.at[0], sa.at[1], up, east), (aa.at[0], sa.at[2], down, east),
        (aa.at[1], sa.at[3], lat, west), (aa.at[1], sa.at[4], up, west), (aa.at[1], sa.at[5], down, west),
        (tt.at[pl.ds(2, 2)], tt.at[pl.ds(rows + 2, 2)], up, lon), (tt.at[pl.ds(rows, 2)], tt.at[pl.ds(0, 2)], down, lon),
    ]
    sent = []
    for i, (src, dst, p, q) in enumerate(halo):
        c = pltpu.make_async_remote_copy(src, dst, h_send.at[i], h_recv.at[i], device_id=(p, q), device_id_type=MESH)
        c.start()
        sent.append(c)
    for a, b in order:
        pltpu.make_async_remote_copy(stat, srecv.at[me], s_send, s_recv,
                                     device_id=(la[a], lo[b]), device_id_type=MESH).start()
    for a, b in order:
        pltpu.make_async_remote_copy(
            nf_hbm.at[0, pl.ds(pl.multiple_of(la[a] * rows, rows), rows), pl.ds(pl.multiple_of(lo[b] * cols, cols), cols)],
            recv.at[me], a_send, a_recv, device_id=(la[a], lo[b]), device_id_type=MESH).start()

    for c in sent:
        c.wait_recv()
    first = lat == 0
    last = lat == n_lat - 1
    for r in (0, 1):
        tt[r] = jnp.where(first, zero, tt[r])
        tt[rows + 2 + r] = jnp.where(last, zero, tt[rows + 2 + r])
    strip = strips(0, 2, strips(rows + 2, rows + 4, (aa[0], aa[1])))
    valid = (lane < 3 * (rows + 4)) & ((lane >= 6) | (lat > 0)) & ((lane < 3 * (rows + 2)) | (lat < n_lat - 1))
    shift = 3 * rows
    west_in = jnp.where(lane < 6, pltpu.roll(sa[2], cols - shift, axis=1),
                        jnp.where(lane < 3 * (rows + 2), sa[0], pltpu.roll(sa[1], shift, axis=1)))
    east_in = jnp.where(lane < 6, pltpu.roll(sa[5], cols - shift, axis=1),
                        jnp.where(lane < 3 * (rows + 2), sa[3], pltpu.roll(sa[4], shift, axis=1)))
    g_west = jnp.where(valid, jnp.where(lane_col == 2, strip[0], west_in), zero)
    g_east = jnp.where(valid, jnp.where(lane_col == 0, strip[1], east_in), zero)
    for a in range(3):
        for b in range(3):
            amount = (-(3 * (a - 1) + b - 1)) % cols
            for s, g in enumerate((g_west, g_east)):
                xe[a, s, KB * b:KB * (b + 1), :] = pltpu.roll(g, amount, axis=1) if amount else g
    for r in range(rows + 4):
        v = tt[r]
        center = 3 * r + 1
        xx[r, 0:KB, :] = jnp.where(lane == 0, pltpu.roll(g_west, (-center) % cols, axis=1), pltpu.roll(v, 1, axis=1))
        xx[r, KB:2 * KB, :] = v
        xx[r, 2 * KB:3 * KB, :] = jnp.where(
            lane == cols - 1, pltpu.roll(g_east, (cols - 1 - center) % cols, axis=1), pltpu.roll(v, cols - 1, axis=1))

    def drain(buf, sem):
        w = buf.at[pl.ds(0, n_dev - 1)]
        pltpu.make_async_copy(w, w, sem).wait()

    drain(srecv, s_recv)
    total = jnp.sum(srecv[...], axis=0) / (n_dev * rows * cols)
    mean = total[0:1, :]
    scale = 1.0 / jnp.sqrt(total[1:2, :] - mean * mean + 1e-05)
    in_use = lax.broadcasted_iota(jnp.int32, (1, cols), 1) < channels

    def beside(v):
        wide = jnp.concatenate([jnp.where(in_use, v, 0.0), jnp.zeros((1, KP - cols), f32)], axis=1)
        return wide + pltpu.roll(wide, KB, axis=1) + pltpu.roll(wide, 2 * KB, axis=1)

    mean_k, scale_k = beside(mean), beside(scale)
    full = bias[0]
    for a in range(3):
        ws = (w1c[a].astype(f32) * scale_k).astype(bf16)
        w1s[a] = ws
        part = jnp.broadcast_to(jnp.sum(ws.astype(f32) * mean_k, axis=1, keepdims=True), (hid_ch, cols))
        full = full - part
        if a != 1:
            bias[2 + a // 2] = part
    bias[0] = full

    top = jnp.where(first, 1.0, 0.0).astype(f32)
    bottom = jnp.where(last, 1.0, 0.0).astype(f32)
    hlane = lax.broadcasted_iota(jnp.int32, (hid_ch, cols), 1)

    def conv1(parts):
        acc = jnp.zeros((hid_ch, cols * len(parts(0))), f32)
        for a in range(3):
            acc = acc + jnp.dot(w1s[a], jnp.concatenate(parts(a), axis=1), preferred_element_type=f32)
        return acc

    def put(r, h):
        hid[1, r] = h
        center = 3 * (r + 1) + 1
        hid[0, r] = jnp.where(hlane == 0, pltpu.roll(edge[0], lax.rem(2 * cols - center, cols), axis=1), pltpu.roll(h, 1, axis=1))
        hid[2, r] = jnp.where(hlane == cols - 1, pltpu.roll(edge[1], lax.rem(2 * cols - 1 - center, cols), axis=1),
                              pltpu.roll(h, cols - 1, axis=1))

    acc = conv1(lambda a: [xe[a, 0], xe[a, 1], xx[rows + a], xx[rows + 1 + a]])
    ebias = (bias[0] + jnp.where((hlane >= 6) & (hlane < 9), top, 0.0) * bias[2]
             + jnp.where((hlane >= 3 * rows + 3) & (hlane < 3 * rows + 6), bottom, 0.0) * bias[3])
    keep = (((hlane >= 6) | (lat > 0)) & ((hlane < 3 * rows + 6) | (lat < n_lat - 1)))
    for s in range(2):
        edge[s] = jnp.where(keep, gelu(acc[:, s * cols:(s + 1) * cols] + ebias), 0.0).astype(bf16)
    put(rows, gelu(acc[:, 2 * cols:3 * cols] + (bias[0] + bottom * bias[3])).astype(bf16))
    put(rows + 1, jnp.where(last, 0.0, gelu(acc[:, 3 * cols:] + bias[0])).astype(bf16))

    def tile1(r0):
        acc = conv1(lambda a: [xx[r0 + a + q] for q in range(4)])
        for q in range(4):
            v = acc[:, q * cols:(q + 1) * cols] + bias[0]
            if r0 == 0 and q == 1:
                v = v + top * bias[2]
            h = gelu(v)
            if r0 == 0 and q == 0:
                h = jnp.where(first, 0.0, h)
            put(r0 + q, h.astype(bf16))

    def tile2(r0):
        acc = jnp.zeros((hid_ch, 4 * cols), f32)
        for a in range(3):
            for b in range(3):
                x = jnp.concatenate([hid[b, r0 + a + q] for q in range(4)], axis=1)
                acc = acc + jnp.dot(w2[3 * a + b], x, preferred_element_type=f32)
        return [acc[:, q * cols:(q + 1) * cols] + bias[1] for q in range(4)]

    loads[4].wait()
    for r0 in (0, 4, 8):
        tile1(r0)
    for g in range(rows // 8):
        for r0 in (8 * g + 12, 8 * g + 16):
            if r0 < rows:
                tile1(r0)
        outs = tile2(8 * g) + tile2(8 * g + 4)
        feat_ref[:, 8 * g:8 * g + 8, :] = jnp.swapaxes(jnp.stack(outs, axis=0), 0, 1).astype(bf16)

    own.wait()
    loads[5].wait()
    drain(recv, a_recv)
    for c in range(channels):
        next_ref[c] = recv[slot[c]]
    for c in sent:
        c.wait_send()
    drain(srecv, s_send)
    drain(recv, a_send)


def solution(mesh):
    n_lat, n_lon = mesh.shape["lat"], mesh.shape["lon"]
    n_dev = n_lat * n_lon

    def body(current, next_fields, reader_slot, first_weight, first_bias, second_weight, second_bias):
        channels, rows, cols = current.shape
        hid_ch = first_weight.shape[1]
        bf16, f32 = jnp.bfloat16, jnp.float32
        dma = pltpu.SemaphoreType.DMA
        return pl.pallas_call(
            functools.partial(kernel, n_lat, n_lon, channels, rows, cols, hid_ch),
            out_shape=(jax.ShapeDtypeStruct((hid_ch, rows, cols), bf16), jax.ShapeDtypeStruct((channels, rows, cols), bf16)),
            in_specs=[pl.BlockSpec(memory_space=pltpu.HBM)] * 7,
            out_specs=(pl.BlockSpec(memory_space=pltpu.VMEM),) * 2,
            scratch_shapes=[
                pltpu.VMEM((channels, rows, cols), bf16),
                pltpu.VMEM((9, channels, hid_ch), bf16),
                pltpu.VMEM(second_weight.shape, bf16),
                pltpu.VMEM((2, 1, hid_ch), f32),
                pltpu.SMEM(reader_slot.shape, jnp.int32),
                pltpu.VMEM((rows + 4, KB, cols), bf16),
                pltpu.VMEM((2, KB, cols), bf16),
                pltpu.VMEM((6, KB, cols), bf16),
                pltpu.VMEM((rows + 4, KP, cols), bf16),
                pltpu.VMEM((3, 2, KP, cols), bf16),
                pltpu.VMEM((3, KP, hid_ch), bf16),
                pltpu.VMEM((3, hid_ch, KP), bf16),
                pltpu.VMEM((4, hid_ch, cols), f32),
                pltpu.VMEM((3, rows + 2, hid_ch, cols), bf16),
                pltpu.VMEM((2, hid_ch, cols), bf16),
                pltpu.VMEM((2, cols), f32),
                pltpu.VMEM((n_dev, 2, cols), f32),
                pltpu.VMEM((n_dev, rows, cols), bf16),
                dma((7,)), dma((8,)), dma((8,)), dma, dma, dma, dma,
            ],
            compiler_params=pltpu.CompilerParams(collective_id=0, has_side_effects=True, vmem_limit_bytes=40 * 1024 * 1024),
        )(*(pltpu.with_memory_space_constraint(v, pltpu.HBM) for v in (
            current, next_fields, reader_slot, jnp.swapaxes(first_weight, 1, 2), first_bias.reshape(1, -1),
            second_weight, second_bias.reshape(1, -1))))

    split = P(None, "lat", "lon")
    return jax.shard_map(
        body,
        mesh=mesh,
        in_specs=(split, P(("lat", "lon"), None, None), P(), P(), P(), P(), P()),
        out_specs=(split, split),
        check_vma=False,
    )
```

```python
import functools
import random

import jax
import jax.numpy as jnp
from jax import lax
from jax.experimental import pallas as pl
from jax.experimental.pallas import tpu as pltpu
from jax.sharding import PartitionSpec as P

MESH = pl.DeviceIdType.MESH
KB = 80
KP = 256


def gelu(v):
    u = v * (0.7978845608028654 + 0.035677408136300125 * (v * v))
    half = 0.5 * v
    return half + half * jnp.tanh(u)


def kernel(n_lat, n_lon, channels, rows, cols, hid_ch,
           cur_hbm, nf_hbm, slot_hbm, w1_hbm, b1_hbm, w2_hbm, b2_hbm,
           feat_ref, next_ref,
           cur, w1, w2, bv, slot, tt, aa, sa, xx, xe, w1c, w1s, bias, hid, edge,
           stat, srecv, recv, in_sem, h_send, h_recv, s_send, s_recv, a_send, a_recv):
    f32, bf16 = jnp.float32, jnp.bfloat16
    n_dev = n_lat * n_lon
    lat = lax.axis_index("lat")
    lon = lax.axis_index("lon")
    me = lat * n_lon + lon
    la = [lax.rem(lat + d, n_lat) for d in range(n_lat)]
    lo = [lax.rem(lon + d, n_lon) for d in range(n_lon)]
    order = [(a, b) for a in range(n_lat) for b in range(n_lon) if (a, b) != (0, 0)]
    random.Random(0).shuffle(order)

    def load(i, src, dst):
        return pltpu.make_async_copy(src, dst, in_sem.at[i])

    loads = [load(0, cur_hbm, cur), load(1, w1_hbm, w1), load(2, b1_hbm, bv.at[0]),
             load(3, b2_hbm, bv.at[1]), load(4, w2_hbm, w2), load(5, slot_hbm, slot)]
    for c in loads:
        c.start()
    own = pltpu.make_async_copy(
        nf_hbm.at[0, pl.ds(pl.multiple_of(lat * rows, rows), rows), pl.ds(pl.multiple_of(lon * cols, cols), cols)],
        recv.at[me], in_sem.at[6])
    own.start()
    barrier = pltpu.get_barrier_semaphore()
    for a, b in order:
        pl.semaphore_signal(barrier, inc=1, device_id=(la[a], lo[b]), device_id_type=MESH)

    tt[2:rows + 2, 64:KB, :] = jnp.zeros((rows, KB - 64, cols), bf16)
    loads[0].wait()
    sum1 = jnp.zeros((channels, cols), f32)
    sum2 = jnp.zeros((channels, cols), f32)
    for h in range(0, rows, 8):
        t = jnp.swapaxes(cur[:, h:h + 8, :].astype(f32), 0, 1)
        sum1 = sum1 + jnp.sum(t, axis=0)
        sum2 = sum2 + jnp.sum(t * t, axis=0)
        tt[2 + h:10 + h, 0:channels, :] = t.astype(bf16)
    diag = lax.broadcasted_iota(jnp.int32, (channels, cols), 0) == lax.broadcasted_iota(jnp.int32, (channels, cols), 1)
    for i, s in enumerate((sum1, sum2)):
        col = jnp.sum(s, axis=1, keepdims=True)
        stat[i:i + 1, :] = jnp.sum(jnp.where(diag, col, 0.0), axis=0, keepdims=True)
    lane = lax.broadcasted_iota(jnp.int32, (KB, cols), 1)
    lane_row = lax.shift_right_logical(lane * 171, 9)
    lane_col = lane - 3 * lane_row

    def strips(first, last, base):
        out = list(base)
        for r in range(first, last):
            v = tt[r]
            for s in range(2):
                out[s] = jnp.where(lane_row == r, pltpu.roll(v, (3 * r + 2 - s) % cols, axis=1), out[s])
        return out

    zero = jnp.zeros((KB, cols), bf16)
    strip = strips(2, rows + 2, (zero, zero))
    aa[0] = strip[0]
    aa[1] = strip[1]
    srecv[me] = stat[...]
    pl.semaphore_wait(barrier, n_dev - 1)

    for a, b in order:
        pltpu.make_async_remote_copy(stat, srecv.at[me], s_send, s_recv,
                                     device_id=(la[a], lo[b]), device_id_type=MESH).start()
    up, down, east, west = la[n_lat - 1], la[1], lo[1], lo[n_lon - 1]
    halo = [
        (aa.at[0], sa.at[0], lat, east), (aa.at[0], sa.at[1], up, east), (aa.at[0], sa.at[2], down, east),
        (aa.at[1], sa.at[3], lat, west), (aa.at[1], sa.at[4], up, west), (aa.at[1], sa.at[5], down, west),
        (tt.at[pl.ds(2, 2)], tt.at[pl.ds(rows + 2, 2)], up, lon), (tt.at[pl.ds(rows, 2)], tt.at[pl.ds(0, 2)], down, lon),
    ]
    sent = []
    for i, (src, dst, p, q) in enumerate(halo):
        c = pltpu.make_async_remote_copy(src, dst, h_send.at[i], h_recv.at[i], device_id=(p, q), device_id_type=MESH)
        c.start()
        sent.append(c)

    loads[1].wait()
    w1c[...] = jnp.zeros_like(w1c)
    for tap in range(9):
        w1c[tap // 3, KB * (tap % 3):KB * (tap % 3) + channels, :] = w1[tap]
    for a in range(3):
        w1c[a] = jnp.transpose(w1c[a])
    xx[:, 3 * KB:KP, :] = jnp.zeros((rows + 4, KP - 3 * KB, cols), bf16)
    xe[:, :, 3 * KB:KP, :] = jnp.zeros((3, 2, KP - 3 * KB, cols), bf16)
    loads[2].wait()
    loads[3].wait()
    eye = lax.broadcasted_iota(jnp.int32, (hid_ch, hid_ch), 0) == lax.broadcasted_iota(jnp.int32, (hid_ch, hid_ch), 1)
    for i in range(2):
        col = jnp.sum(jnp.where(eye, bv[i], 0.0), axis=1, keepdims=True)
        bias[i] = jnp.broadcast_to(col, (hid_ch, cols))

    for c in sent:
        c.wait_recv()
    for a, b in order:
        pltpu.make_async_remote_copy(
            nf_hbm.at[0, pl.ds(pl.multiple_of(la[a] * rows, rows), rows), pl.ds(pl.multiple_of(lo[b] * cols, cols), cols)],
            recv.at[me], a_send, a_recv, device_id=(la[a], lo[b]), device_id_type=MESH).start()

    first = lat == 0
    last = lat == n_lat - 1
    for r in (0, 1):
        tt[r] = jnp.where(first, zero, tt[r])
        tt[rows + 2 + r] = jnp.where(last, zero, tt[rows + 2 + r])
    strip = strips(0, 2, strips(rows + 2, rows + 4, (aa[0], aa[1])))
    valid = (lane < 3 * (rows + 4)) & ((lane >= 6) | (lat > 0)) & ((lane < 3 * (rows + 2)) | (lat < n_lat - 1))
    shift = 3 * rows
    west_in = jnp.where(lane < 6, pltpu.roll(sa[2], cols - shift, axis=1),
                        jnp.where(lane < 3 * (rows + 2), sa[0], pltpu.roll(sa[1], shift, axis=1)))
    east_in = jnp.where(lane < 6, pltpu.roll(sa[5], cols - shift, axis=1),
                        jnp.where(lane < 3 * (rows + 2), sa[3], pltpu.roll(sa[4], shift, axis=1)))
    g_west = jnp.where(valid, jnp.where(lane_col == 2, strip[0], west_in), zero)
    g_east = jnp.where(valid, jnp.where(lane_col == 0, strip[1], east_in), zero)
    for a in range(3):
        for b in range(3):
            amount = (-(3 * (a - 1) + b - 1)) % cols
            for s, g in enumerate((g_west, g_east)):
                xe[a, s, KB * b:KB * (b + 1), :] = pltpu.roll(g, amount, axis=1) if amount else g
    for r in range(rows + 4):
        v = tt[r]
        center = 3 * r + 1
        xx[r, 0:KB, :] = jnp.where(lane == 0, pltpu.roll(g_west, (-center) % cols, axis=1), pltpu.roll(v, 1, axis=1))
        xx[r, KB:2 * KB, :] = v
        xx[r, 2 * KB:3 * KB, :] = jnp.where(
            lane == cols - 1, pltpu.roll(g_east, (cols - 1 - center) % cols, axis=1), pltpu.roll(v, cols - 1, axis=1))

    def drain(buf, sem):
        w = buf.at[pl.ds(0, n_dev - 1)]
        pltpu.make_async_copy(w, w, sem).wait()

    drain(srecv, s_recv)
    total = jnp.sum(srecv[...], axis=0) / (n_dev * rows * cols)
    mean = total[0:1, :]
    scale = 1.0 / jnp.sqrt(total[1:2, :] - mean * mean + 1e-05)
    in_use = lax.broadcasted_iota(jnp.int32, (1, cols), 1) < channels

    def beside(v):
        wide = jnp.concatenate([jnp.where(in_use, v, 0.0), jnp.zeros((1, KP - cols), f32)], axis=1)
        return wide + pltpu.roll(wide, KB, axis=1) + pltpu.roll(wide, 2 * KB, axis=1)

    mean_k, scale_k = beside(mean), beside(scale)
    full = bias[0]
    for a in range(3):
        ws = (w1c[a].astype(f32) * scale_k).astype(bf16)
        w1s[a] = ws
        part = jnp.broadcast_to(jnp.sum(ws.astype(f32) * mean_k, axis=1, keepdims=True), (hid_ch, cols))
        full = full - part
        if a != 1:
            bias[2 + a // 2] = part
    bias[0] = full

    top = jnp.where(first, 1.0, 0.0).astype(f32)
    bottom = jnp.where(last, 1.0, 0.0).astype(f32)
    hlane = lax.broadcasted_iota(jnp.int32, (hid_ch, cols), 1)

    def conv1(parts):
        acc = jnp.zeros((hid_ch, cols * len(parts(0))), f32)
        for a in range(3):
            acc = acc + jnp.dot(w1s[a], jnp.concatenate(parts(a), axis=1), preferred_element_type=f32)
        return acc

    def put(r, h):
        hid[1, r] = h
        center = 3 * (r + 1) + 1
        hid[0, r] = jnp.where(hlane == 0, pltpu.roll(edge[0], lax.rem(2 * cols - center, cols), axis=1), pltpu.roll(h, 1, axis=1))
        hid[2, r] = jnp.where(hlane == cols - 1, pltpu.roll(edge[1], lax.rem(2 * cols - 1 - center, cols), axis=1),
                              pltpu.roll(h, cols - 1, axis=1))

    acc = conv1(lambda a: [xe[a, 0], xe[a, 1], xx[rows + a], xx[rows + 1 + a]])
    ebias = (bias[0] + jnp.where((hlane >= 6) & (hlane < 9), top, 0.0) * bias[2]
             + jnp.where((hlane >= 3 * rows + 3) & (hlane < 3 * rows + 6), bottom, 0.0) * bias[3])
    keep = (((hlane >= 6) | (lat > 0)) & ((hlane < 3 * rows + 6) | (lat < n_lat - 1)))
    for s in range(2):
        edge[s] = jnp.where(keep, gelu(acc[:, s * cols:(s + 1) * cols] + ebias), 0.0).astype(bf16)
    put(rows, gelu(acc[:, 2 * cols:3 * cols] + (bias[0] + bottom * bias[3])).astype(bf16))
    put(rows + 1, jnp.where(last, 0.0, gelu(acc[:, 3 * cols:] + bias[0])).astype(bf16))

    def tile1(r0):
        acc = conv1(lambda a: [xx[r0 + a + q] for q in range(4)])
        for q in range(4):
            v = acc[:, q * cols:(q + 1) * cols] + bias[0]
            if r0 == 0 and q == 1:
                v = v + top * bias[2]
            h = gelu(v)
            if r0 == 0 and q == 0:
                h = jnp.where(first, 0.0, h)
            put(r0 + q, h.astype(bf16))

    def tile2(r0):
        acc = jnp.zeros((hid_ch, 4 * cols), f32)
        for a in range(3):
            for b in range(3):
                x = jnp.concatenate([hid[b, r0 + a + q] for q in range(4)], axis=1)
                acc = acc + jnp.dot(w2[3 * a + b], x, preferred_element_type=f32)
        return [acc[:, q * cols:(q + 1) * cols] + bias[1] for q in range(4)]

    loads[4].wait()
    for r0 in (0, 4, 8):
        tile1(r0)
    for g in range(rows // 8):
        for r0 in (8 * g + 12, 8 * g + 16):
            if r0 < rows:
                tile1(r0)
        outs = tile2(8 * g) + tile2(8 * g + 4)
        feat_ref[:, 8 * g:8 * g + 8, :] = jnp.swapaxes(jnp.stack(outs, axis=0), 0, 1).astype(bf16)

    own.wait()
    loads[5].wait()
    drain(recv, a_recv)
    for c in range(channels):
        next_ref[c] = recv[slot[c]]
    for c in sent:
        c.wait_send()
    drain(srecv, s_send)
    drain(recv, a_send)


def solution(mesh):
    n_lat, n_lon = mesh.shape["lat"], mesh.shape["lon"]
    n_dev = n_lat * n_lon

    def body(current, next_fields, reader_slot, first_weight, first_bias, second_weight, second_bias):
        channels, rows, cols = current.shape
        hid_ch = first_weight.shape[1]
        bf16, f32 = jnp.bfloat16, jnp.float32
        dma = pltpu.SemaphoreType.DMA
        return pl.pallas_call(
            functools.partial(kernel, n_lat, n_lon, channels, rows, cols, hid_ch),
            out_shape=(jax.ShapeDtypeStruct((hid_ch, rows, cols), bf16), jax.ShapeDtypeStruct((channels, rows, cols), bf16)),
            in_specs=[pl.BlockSpec(memory_space=pltpu.HBM)] * 7,
            out_specs=(pl.BlockSpec(memory_space=pltpu.VMEM),) * 2,
            scratch_shapes=[
                pltpu.VMEM((channels, rows, cols), bf16),
                pltpu.VMEM((9, channels, hid_ch), bf16),
                pltpu.VMEM(second_weight.shape, bf16),
                pltpu.VMEM((2, 1, hid_ch), f32),
                pltpu.SMEM(reader_slot.shape, jnp.int32),
                pltpu.VMEM((rows + 4, KB, cols), bf16),
                pltpu.VMEM((2, KB, cols), bf16),
                pltpu.VMEM((6, KB, cols), bf16),
                pltpu.VMEM((rows + 4, KP, cols), bf16),
                pltpu.VMEM((3, 2, KP, cols), bf16),
                pltpu.VMEM((3, KP, hid_ch), bf16),
                pltpu.VMEM((3, hid_ch, KP), bf16),
                pltpu.VMEM((4, hid_ch, cols), f32),
                pltpu.VMEM((3, rows + 2, hid_ch, cols), bf16),
                pltpu.VMEM((2, hid_ch, cols), bf16),
                pltpu.VMEM((2, cols), f32),
                pltpu.VMEM((n_dev, 2, cols), f32),
                pltpu.VMEM((n_dev, rows, cols), bf16),
                dma((7,)), dma((8,)), dma((8,)), dma, dma, dma, dma,
            ],
            compiler_params=pltpu.CompilerParams(collective_id=0, has_side_effects=True, vmem_limit_bytes=40 * 1024 * 1024),
        )(*(pltpu.with_memory_space_constraint(v, pltpu.HBM) for v in (
            current, next_fields, reader_slot, jnp.swapaxes(first_weight, 1, 2), first_bias.reshape(1, -1),
            second_weight, second_bias.reshape(1, -1))))

    split = P(None, "lat", "lon")
    return jax.shard_map(
        body,
        mesh=mesh,
        in_specs=(split, P(("lat", "lon"), None, None), P(), P(), P(), P(), P()),
        out_specs=(split, split),
        check_vma=False,
    )
```
